256 devices in a mesh: grp: 2 (over z), row: 16 (over x, core), col: 8 (over y).
Axes of the slice: x: 8, y: 8, z: 2, core: 2. Of those that a mesh axis runs over, the one named last changes fastest.
The devices are a block of a 8x8x16 slice.
Arguments:
- perturbation: bfloat16 [4, 12000, 12000], P('grp', 'row', 'col'), parts along dimension 0, may hold values from -96 to 96
- occ_coeffs: bfloat16 [12000, 2000], P('row', 'col'), may hold values from -0.0546875 to 0.0546875
- vir_coeffs: bfloat16 [12000, 512], P('col', 'row'), may hold values from -0.0546875 to 0.0546875
- occ_energies: float32 [2000], replicated, may hold values from -1 to -0.1
- vir_energies: float32 [512], replicated, may hold values from 0.1 to 1.5
Outputs:
- density_response: bfloat16 [4, 12000, 12000], P('grp', 'row', 'col'), parts along dimension 0
The draws below stay inside these ranges and needn't reach their ends.
There are 2 independent parts, one for each index of `grp`. The reference program is written for one: setup_inputs(seed, part) draws one part's arguments, and reference() takes and returns one part's arrays. A program takes and returns all parts, laid end to end along the dimension named above; an argument that names none is the same for every part. Nothing has to cross between parts.
All inputs are finite; a program needn't handle non-finite values.
Results may differ from the reference program's by a relative error of at most 0.0098.
Values may be sent and summed in bfloat16 or wider, within the bound.
No kernel may reach another device: no remote copies, remote signals or barrier semaphores. Data moves between devices by JAX's collectives and lax.ppermute only.
A program may use at most 64 MiB of HBM per device.

```python
import jax
import jax.numpy as jnp
from jax import lax

NB = 12000
NOCC = 2000
NV = 512
PERT = 2


def block_levels(rng, shape, cuts, smallest, high):
    factor_of = 1.0
    for dim, shards_of in cuts:
        draws = jax.random.uniform(jax.random.fold_in(jax.random.fold_in(rng, 6), dim), (shards_of,), jnp.float32, smallest / len(cuts), high / len(cuts))
        factor_of = factor_of * jnp.repeat(jnp.exp(draws), shape[dim] // shards_of).reshape((-1,) + (1,) * (len(shape) - 1 - dim))
    return factor_of


def scatter_about(key, shape, spread, bound, cuts=(), held_as=jnp.bfloat16):
    array = spread * jax.random.normal(key, shape, jnp.float32)
    if cuts:
        array = array * block_levels(key, shape, cuts, -0.22, 0.18)
    return jnp.clip(array, -bound, bound).astype(held_as)


def setup_inputs(seed: int = 0, part: int = 0) -> dict:
    seeds = jax.random.split(jax.random.key(seed), 6)
    part_keys = jax.random.split(jax.random.fold_in(seeds[5], part), 6)
    return {
        "perturbation": scatter_about(part_keys[0], (PERT, NB, NB), 16.0, 96.0, ((1, 16), (2, 8))),
        "occ_coeffs": scatter_about(seeds[1], (NB, NOCC), NB ** -0.5, 0.0546875, ((0, 16), (1, 8))),
        "vir_coeffs": scatter_about(seeds[2], (NB, NV), NB ** -0.5, 0.0546875, ((0, 8), (1, 16))),
        "occ_energies": jnp.clip(jax.random.uniform(seeds[3], (NOCC,), jnp.float32, -1.0, -0.1), -1.0, -0.1),
        "vir_energies": jnp.clip(jax.random.uniform(seeds[4], (NV,), jnp.float32, 0.1, 1.5), 0.1, 1.5),
    }


def reference(perturbation, occ_coeffs, vir_coeffs, occ_energies, vir_energies):
    gaps = occ_energies[:, None] - vir_energies[None, :]
    occ_wide = occ_coeffs.astype(jnp.float32)
    results = []
    for index in range(PERT):
        image = jnp.dot(perturbation[index], vir_coeffs, preferred_element_type=jnp.float32)
        coupling = jnp.dot(occ_wide.T, image, precision=lax.Precision.HIGHEST)
        response = (coupling / gaps).astype(jnp.bfloat16)
        mixed = jnp.dot(occ_coeffs, response, preferred_element_type=jnp.float32).astype(jnp.bfloat16)
        results.append(jnp.dot(mixed, vir_coeffs.T, preferred_element_type=jnp.float32).astype(jnp.bfloat16))
    return jnp.stack(results)
```

```python
import jax
import jax.numpy as jnp
from jax import lax
from jax.sharding import Mesh
from jax.sharding import PartitionSpec as P

CORES = 2
LANES = 128
SUBLANES = 8
SWAP = [(0, 1), (1, 0)]


def turn(shard, axis, step):
    size = lax.axis_size(axis)
    return lax.ppermute(shard, axis, [(i, (i + step) % size) for i in range(size)])


def middle(shard):
    return -(-shard.shape[0] // (2 * SUBLANES)) * SUBLANES


def ring_gather(shard, axis):
    half = lax.axis_size(axis) // 2
    pieces, down, up = [shard], shard, shard
    for _ in range(half - 1):
        down, up = turn(down, axis, 1), turn(up, axis, -1)
        pieces += [down, up]
    mid = middle(shard)
    far = [turn(down[:mid], axis, 1), turn(up[mid:], axis, -1)]
    return pieces + [jnp.concatenate(far, axis=0)]


def ring_order(axis):
    half = lax.axis_size(axis) // 2
    steps = [0]
    for s in range(1, half):
        steps += [-s, s]
    return steps + [half]


def ring_scatter_sum(piece, axis):
    half = lax.axis_size(axis) // 2
    far = piece(half)
    mid = middle(far)
    down, up = turn(far[:mid], axis, 1), turn(far[mid:], axis, -1)
    down = jnp.pad(down, [(0, len(far) - mid), (0, 0)])
    up = jnp.pad(up, [(mid, 0), (0, 0)])
    for d in range(half - 1, 0, -1):
        wide = [piece(d).astype(jnp.float32) + down, piece(-d).astype(jnp.float32) + up]
        down, up = turn(wide[0].astype(jnp.bfloat16), axis, 1), turn(wide[1].astype(jnp.bfloat16), axis, -1)
    return piece(0).astype(jnp.float32) + down + up


def exchanged(pieces, axis):
    return lax.all_to_all(pieces, axis, split_axis=0, concat_axis=0, tiled=True)


def per_device(perturbation, occ_coeffs, vir_coeffs, occ_energies, vir_energies):
    nx, ny = lax.axis_size("x"), lax.axis_size("y")
    x, k, y = (lax.axis_index(a) for a in ("x", "k", "y"))
    perts, rows, cols = perturbation.shape
    wide = jnp.float32
    narrow = jnp.bfloat16

    vir = vir_coeffs.T
    own = exchanged(jnp.broadcast_to(vir, (nx, *vir.shape)), "x").reshape(-1, cols)
    other = lax.ppermute(own, "k", SWAP)

    occ_own = occ_coeffs.shape[1]
    padded = -(-occ_own // LANES) * LANES
    occ = ring_gather(jnp.pad(occ_coeffs, [(0, 0), (0, padded - occ_own)]), "y")
    occ = jnp.concatenate(occ, axis=1)

    parts = own.shape[0] // LANES
    image = []
    for v in (own, other):
        block = jnp.einsum("pij,bvj->pbiv", perturbation, v.reshape(parts, LANES, cols), preferred_element_type=wide)
        image.append(block.astype(narrow))
    image = jnp.stack(image, axis=1).reshape(-1, rows, LANES)

    def place(member):
        member = member % ny
        p, core, part = member // (CORES * parts), member // parts % CORES, member % parts
        return (p * CORES + (core ^ k)) * parts + part

    def piece(d):
        return lax.dynamic_index_in_dim(image, place(y + d), 0, keepdims=False)

    image = ring_scatter_sum(piece, "y").astype(narrow)
    value = jnp.einsum("io,iv->ov", occ, image, preferred_element_type=wide)
    value = value.reshape(CORES, -1, LANES)
    mine = lax.dynamic_index_in_dim(value, k, 0, keepdims=False)
    yours = lax.dynamic_index_in_dim(value, 1 - k, 0, keepdims=False).astype(narrow)
    mine = mine + lax.ppermute(yours, "k", SWAP).astype(wide)
    share = mine.shape[0] // nx
    mine = exchanged(mine.astype(narrow).reshape(nx, share, LANES), "x")
    coupling = jnp.sum(mine.astype(wide), axis=0)

    levels = jnp.pad(occ_energies.reshape(ny, occ_own), [(0, 0), (0, padded - occ_own)], constant_values=-1.0)
    members = (y + jnp.array(ring_order("y"))) % ny
    levels = jnp.take(levels, members, axis=0).reshape(-1)
    levels = lax.dynamic_slice_in_dim(levels, (k * nx + x) * share, share)
    virtual = vir_energies.reshape(parts, nx // parts, CORES, -1)
    virtual = jnp.moveaxis(virtual, 2, 0).reshape(CORES * parts, LANES)
    virtual = lax.dynamic_index_in_dim(virtual, y % (CORES * parts), 0, keepdims=False)
    response = (coupling / (levels[:, None] - virtual[None, :])).astype(narrow)

    response = exchanged(jnp.broadcast_to(response, (nx, *response.shape)), "x").reshape(-1, LANES)
    sibling = lax.ppermute(response, "k", SWAP)
    low, high = jnp.where(k == 0, response, sibling), jnp.where(k == 0, sibling, response)
    response = jnp.concatenate([low, high], axis=0)
    mixed = jnp.dot(occ, response, preferred_element_type=wide).astype(narrow)

    mixed = jnp.stack(ring_gather(mixed, "y"))
    order = ring_order("y")
    at = jnp.array([order.index((d + ny // 2 - 1) % ny - ny // 2 + 1) for d in range(ny)])
    picks = []
    for p in range(perts):
        for rel in range(CORES):
            for part in range(parts):
                member = (p * CORES + (rel ^ k)) * parts + part
                picks.append(lax.dynamic_index_in_dim(mixed, at[(member - y) % ny], 0, keepdims=False))
    vir = jnp.concatenate([own, other], axis=0)
    blocks = CORES * parts
    total = []
    for p in range(perts):
        side = jnp.concatenate(picks[p * blocks : (p + 1) * blocks], axis=1)
        total.append(side)
    total = jnp.einsum("piv,vj->pij", jnp.stack(total), vir, preferred_element_type=wide)
    return total.astype(narrow)


def solution(mesh):
    rows, cols = mesh.shape["row"], mesh.shape["col"]
    torus = Mesh(
        mesh.devices.reshape(mesh.shape["grp"], rows // CORES, CORES, cols),
        ("grp", "x", "k", "y"),
    )
    row = ("x", "k")
    in_specs = (P("grp", row, "y"), P(row, "y"), P("y", row), P(), P())
    return jax.shard_map(
        per_device, mesh=torus, in_specs=in_specs, out_specs=P("grp", row, "y"), check_vma=False
    )
```

```python
import jax
import jax.numpy as jnp
from jax import lax
from jax.experimental import pallas as pl
from jax.experimental.pallas import tpu as pltpu
from jax.sharding import Mesh
from jax.sharding import PartitionSpec as P

CORES = 2
LANES = 128
SWAP = [(0, 1), (1, 0)]
WIDE, NARROW = jnp.float32, jnp.bfloat16
ROOMY = pltpu.CompilerParams(vmem_limit_bytes=20 * 2**20)
SCALAR = pl.BlockSpec(memory_space=pltpu.SMEM)


def up_to(size, unit):
    return -(-size // unit) * unit


def shape_of(*dims, dtype=NARROW):
    return jax.ShapeDtypeStruct(dims, dtype)


def turn(shard, axis, step):
    size = lax.axis_size(axis)
    return lax.ppermute(shard, axis, [(i, (i + step) % size) for i in range(size)])


def ring_gather(shard, axis, mid):
    half = lax.axis_size(axis) // 2
    pieces, down, up = [shard], shard, shard
    for _ in range(half - 1):
        down, up = turn(down, axis, 1), turn(up, axis, -1)
        pieces += [down, up]
    far = [turn(down[:mid], axis, 1), turn(up[mid:], axis, -1)]
    return pieces + far


def ring_order(size):
    steps = [0]
    for s in range(1, size // 2):
        steps += [size - s, s]
    return steps + [size // 2]


def exchanged(pieces, axis):
    return lax.all_to_all(pieces, axis, split_axis=0, concat_axis=0, tiled=True)


def dot(a, b, over):
    return lax.dot_general(a, b, ((over[:1], over[1:]), ((), ())), preferred_element_type=WIDE)


def image_kernel(at, own, other, pert, turned, first, last, *near):
    y, k = at[0], at[1]
    size, share, _ = own.shape
    for d in range(size):
        source = lax.rem(y + d, size)
        for core, held in ((k, own), (1 - k, other)):
            start = pl.multiple_of((CORES * d + core) * share, share)
            turned[pl.ds(start, share), :] = held[source]
    block = CORES * share
    for p in range(pert.shape[0]):
        image = dot(turned[...], pert[p], (1, 1)).astype(NARROW)
        for d in range(size):
            part = image[d * block : (d + 1) * block]
            if d == size // 2:
                (first, last)[p][...] = part
            else:
                near[d - (d > size // 2)][p * block : (p + 1) * block, :] = part


def coupling_kernel(at, here, down, up, *refs):
    *chunks, far_low, far_high, send, keep, image = refs
    k = at[1]
    image[...] = (here[...].astype(WIDE) + down[...].astype(WIDE) + up[...].astype(WIDE)).astype(NARROW)
    block = image.shape[0] // CORES
    held = [image[pl.ds(pl.multiple_of(c * block, block), block), :] for c in (1 - k, k)]
    left = jnp.concatenate(held, axis=0)
    chunks = [c[...] for c in chunks] + [jnp.concatenate([far_low[...], far_high[...]], axis=0)]
    width = chunks[0].shape[1]
    spare = send.shape[2] - width
    for n, chunk in enumerate(chunks):
        value = dot(left, chunk, (1, 0))
        send[n, :, :width] = value[:block].astype(NARROW)
        keep[n, :, :width] = value[block:]
        send[n, :, width:] = jnp.zeros((block, spare), NARROW)
        keep[n, :, width:] = jnp.zeros((block, spare), WIDE)


def response_kernel(terms, levels, virtual, out):
    coupling = terms[0].astype(WIDE)
    for n in range(1, terms.shape[0]):
        coupling += terms[n].astype(WIDE)
    response = (coupling / (levels[...] - virtual[...])).astype(NARROW)
    for n in range(out.shape[0]):
        out[n] = response


def mixed_kernel(at, own, other, *refs):
    *chunks, far_low, far_high, out = refs
    k = at[1]
    chunks = [c[...] for c in chunks] + [jnp.concatenate([far_low[...], far_high[...]], axis=0)]
    width = chunks[0].shape[1]
    total = 0.0
    for n, chunk in enumerate(chunks):
        left = jnp.concatenate([own[n], other[n]], axis=0)[:, :width]
        total += dot(left, chunk, (1, 1))
    block = own.shape[1]
    total = total.astype(NARROW)
    for core, part in ((k, total[:block]), (1 - k, total[block:])):
        out[pl.ds(pl.multiple_of(core * block, block), block), :] = part


def density_kernel(turned, *refs):
    *pieces, first, last, out = refs
    size = len(pieces) + 1
    block = first.shape[0]
    for p in range(out.shape[1]):
        at_block = {d: piece[p * block : (p + 1) * block, :] for d, piece in zip(ring_order(size), pieces)}
        at_block[size // 2] = (first, last)[p][...]
        left = jnp.concatenate([at_block[d] for d in range(size)], axis=0)
        out[:, p, :] = dot(left, turned[...], (0, 0)).astype(NARROW)


def per_device(perturbation, occ_coeffs, vir_coeffs, occ_energies, vir_energies):
    nx, ny = lax.axis_size("x"), lax.axis_size("y")
    x, k, y = (lax.axis_index(a) for a in ("x", "k", "y"))
    perts, rows, cols = perturbation.shape
    own_occ = occ_coeffs.shape[1]
    share = vir_coeffs.shape[1]
    block = CORES * share
    at = jnp.stack([y, k]).astype(jnp.int32)

    mid = up_to(rows // 2, LANES)
    occ = ring_gather(occ_coeffs, "y", mid)
    own = exchanged(jnp.broadcast_to(vir_coeffs.T, (nx, share, cols)), "x")
    other = lax.ppermute(own, "k", SWAP)

    piece = shape_of(perts * block, rows)
    half = shape_of(block, rows)
    turned, first, last, *near = pl.pallas_call(
        image_kernel,
        in_specs=[SCALAR] + [pl.BlockSpec(memory_space=pltpu.VMEM)] * 3,
        out_shape=[shape_of(ny * block, cols), half, half] + [piece] * (ny - 1),
        compiler_params=ROOMY,
    )(at, own, other, perturbation)
    down, up = turn(first, "y", 1), turn(last, "y", -1)
    down = jnp.pad(down, [(0, block), (0, 0)])
    up = jnp.pad(up, [(block, 0), (0, 0)])
    for d in range(ny // 2 - 1, 0, -1):
        down = turn((near[d].astype(WIDE) + down).astype(NARROW), "y", 1)
        up = turn((near[-d].astype(WIDE) + up).astype(NARROW), "y", -1)

    wide_occ = up_to(own_occ, LANES)
    send, keep = pl.pallas_call(
        coupling_kernel,
        in_specs=[SCALAR] + [pl.BlockSpec(memory_space=pltpu.VMEM)] * (3 + len(occ)),
        out_shape=[shape_of(ny, block, wide_occ), shape_of(ny, block, wide_occ, dtype=WIDE)],
        scratch_shapes=[pltpu.VMEM((perts * block, rows), NARROW)],
        compiler_params=ROOMY,
    )(at, near[0], down, up, *occ)
    terms = (keep + lax.ppermute(send, "k", SWAP)).astype(NARROW)
    terms = exchanged(terms, "x")

    chunk = (y + jnp.array(ring_order(ny), jnp.int32)[x]) % ny
    levels = jnp.pad(occ_energies.reshape(ny, own_occ), [(0, 0), (0, wide_occ - own_occ)], constant_values=-1.0)
    levels = lax.dynamic_slice_in_dim(levels, chunk, 1, 0)
    virtual = lax.dynamic_slice_in_dim(vir_energies, y * block, block, 0)[:, None]
    response = pl.pallas_call(
        response_kernel, out_shape=shape_of(nx, block, wide_occ), compiler_params=ROOMY
    )(terms, levels, virtual)
    response = exchanged(response, "x")
    sibling = lax.ppermute(response, "k", SWAP)
    mixed = pl.pallas_call(
        mixed_kernel,
        in_specs=[SCALAR] + [pl.BlockSpec(memory_space=pltpu.VMEM)] * (2 + len(occ)),
        out_shape=piece,
        compiler_params=ROOMY,
    )(at, response, sibling, *occ)

    pieces = ring_gather(mixed, "y", block)
    tile = 2 * LANES
    narrow = [pl.BlockSpec((p.shape[0], tile), lambda i: (0, i)) for p in pieces]
    total = pl.pallas_call(
        density_kernel,
        grid=(pl.cdiv(rows, tile),),
        in_specs=[pl.BlockSpec(turned.shape, lambda i: (0, 0))] + narrow,
        out_specs=pl.BlockSpec((tile, perts, cols), lambda i: (i, 0, 0)),
        out_shape=shape_of(rows, perts, cols),
        compiler_params=ROOMY,
    )(turned, *pieces)
    return jnp.transpose(total, (1, 0, 2))


def solution(mesh):
    rows, cols = mesh.shape["row"], mesh.shape["col"]
    torus = Mesh(
        mesh.devices.reshape(mesh.shape["grp"], rows // CORES, CORES, cols),
        ("grp", "x", "k", "y"),
    )
    row = ("x", "k")
    in_specs = (P("grp", row, "y"), P(row, "y"), P("y", row), P(), P())

    return jax.shard_map(per_device, mesh=torus, in_specs=in_specs, out_specs=P("grp", row, "y"), check_vma=False)
```

```python
import functools

import jax
import jax.numpy as jnp
from jax import lax
from jax.experimental import pallas as pl
from jax.experimental.pallas import tpu as pltpu
from jax.sharding import Mesh
from jax.sharding import PartitionSpec as P

CORES = 2
LANES = 128
SWAP = [(0, 1), (1, 0)]
WIDE, NARROW = jnp.float32, jnp.bfloat16
ROOMY = pltpu.CompilerParams(vmem_limit_bytes=20 * 2**20)
SCALAR = pl.BlockSpec(memory_space=pltpu.SMEM)


def up_to(size, unit):
    return -(-size // unit) * unit


def shape_of(*dims, dtype=NARROW):
    return jax.ShapeDtypeStruct(dims, dtype)


def turn(shard, axis, step):
    size = lax.axis_size(axis)
    return lax.ppermute(shard, axis, [(i, (i + step) % size) for i in range(size)])


def ring_gather(shard, axis, mid):
    half = lax.axis_size(axis) // 2
    pieces, down, up = [shard], shard, shard
    for _ in range(half - 1):
        down, up = turn(down, axis, 1), turn(up, axis, -1)
        pieces += [down, up]
    far = [turn(down[:mid], axis, 1), turn(up[mid:], axis, -1)]
    return pieces + far


def ring_order(size):
    steps = [0]
    for s in range(1, size // 2):
        steps += [size - s, s]
    return steps + [size // 2]


def exchanged(pieces, axis):
    return lax.all_to_all(pieces, axis, split_axis=0, concat_axis=0, tiled=True)


def dot(a, b, over):
    return lax.dot_general(a, b, ((over[:1], over[1:]), ((), ())), preferred_element_type=WIDE)


def turn_and_multiply(at, held, pert, turned, image):
    size, share, _ = held.shape
    for d in range(size):
        turned[d * share : (d + 1) * share, :] = held[lax.rem(at[0] + d, size)]
    for p in range(pert.shape[0]):
        image[p] = dot(turned[...], pert[p], (1, 1)).astype(NARROW)


def own_image_kernel(at, held, pert, turned, image):
    turn_and_multiply(at, held, pert, turned, image)


def image_kernel(at, held, pert, own_image, turned, first, last, *refs):
    *near, image = refs
    turn_and_multiply(at, held, pert, turned, image)
    k = at[1]
    size, share, _ = held.shape
    for p in range(pert.shape[0]):
        for d in range(size):
            for core, source in ((k, own_image), (1 - k, image)):
                part = source[p, d * share : (d + 1) * share, :]
                start = pl.multiple_of(core * share, share)
                if d == size // 2:
                    (first, last)[p][pl.ds(start, share), :] = part
                else:
                    near[d - (d > size // 2)][pl.ds(CORES * p * share + start, share), :] = part


def coupling_kernel(at, here, down, up, *refs):
    *chunks, far_low, far_high, send, keep, far, image = refs
    k = at[1]
    far[: far_low.shape[0], :] = far_low[...]
    far[far_low.shape[0] :, :] = far_high[...]
    image[...] = (here[...].astype(WIDE) + down[...].astype(WIDE) + up[...].astype(WIDE)).astype(NARROW)
    block = image.shape[0] // CORES
    held = [image[pl.ds(pl.multiple_of(c * block, block), block), :] for c in (1 - k, k)]
    left = jnp.concatenate(held, axis=0)
    chunks = [c[...] for c in (*chunks, far)]
    width = chunks[0].shape[1]
    spare = send.shape[2] - width
    for n, chunk in enumerate(chunks):
        value = dot(left, chunk, (1, 0))
        send[n, :, :width] = value[:block].astype(NARROW)
        keep[n, :, :width] = value[block:]
        send[n, :, width:] = jnp.zeros((block, spare), NARROW)
        keep[n, :, width:] = jnp.zeros((block, spare), WIDE)


def response_kernel(terms, levels, virtual, out):
    coupling = terms[0].astype(WIDE)
    for n in range(1, terms.shape[0]):
        coupling += terms[n].astype(WIDE)
    response = (coupling / (levels[...] - virtual[...])).astype(NARROW)
    for n in range(out.shape[0]):
        out[n] = response


def mixed_kernel(at, own, other, *refs):
    *chunks, out = refs
    k = at[1]
    chunks = [c[...] for c in chunks]
    width = chunks[0].shape[1]
    total = 0.0
    for n, chunk in enumerate(chunks):
        left = jnp.concatenate([own[n], other[n]], axis=0)[:, :width]
        total += dot(left, chunk, (1, 1))
    block = own.shape[1]
    total = total.astype(NARROW)
    for core, part in ((k, total[:block]), (1 - k, total[block:])):
        out[pl.ds(pl.multiple_of(core * block, block), block), :] = part


def density_kernel(at, turned, other_turned, *refs):
    *pieces, first, last, out = refs
    k = at[1]
    size = len(pieces) + 1
    share = turned.shape[0] // size
    tile, rows = out.shape[0], first.shape[1]

    def stretch(low, high):
        for p in range(out.shape[1]):
            total = 0.0
            for core, right in ((k, turned), (1 - k, other_turned)):
                start = pl.multiple_of(core * share, share)
                near = pl.ds(CORES * p * share + start, share)
                at_block = {d: piece[near, low:high] for d, piece in zip(ring_order(size), pieces)}
                at_block[size // 2] = (first, last)[p][pl.ds(start, share), low:high]
                left = jnp.concatenate([at_block[d] for d in range(size)], axis=0)
                total += dot(left, right[...], (0, 0))
            out[: high - low, p, :] = total.astype(NARROW)

    for n, low in enumerate(range(0, rows, tile)):
        pl.when(pl.program_id(0) == n)(functools.partial(stretch, low, min(low + tile, rows)))


def per_device(perturbation, occ_coeffs, vir_coeffs, occ_energies, vir_energies):
    nx, ny = lax.axis_size("x"), lax.axis_size("y")
    x, k, y = (lax.axis_index(a) for a in ("x", "k", "y"))
    perts, rows, cols = perturbation.shape
    own_occ = occ_coeffs.shape[1]
    share = vir_coeffs.shape[1]
    block = CORES * share
    at = jnp.stack([y, k]).astype(jnp.int32)

    mid = up_to(rows // 2, LANES)
    occ = ring_gather(occ_coeffs, "y", mid)
    own = exchanged(jnp.broadcast_to(vir_coeffs.T, (nx, share, cols)), "x")
    other = lax.ppermute(own, "k", SWAP)

    piece = shape_of(perts * block, rows)
    half = shape_of(block, rows)
    kept = pl.BlockSpec(memory_space=pltpu.VMEM)
    some = shape_of(nx * share, cols)
    turned, own_image = pl.pallas_call(
        own_image_kernel,
        in_specs=[SCALAR, kept, kept],
        out_specs=[kept, kept],
        out_shape=[some, shape_of(perts, nx * share, rows)],
        compiler_params=ROOMY,
    )(at, own, perturbation)
    other_turned, first, last, *near = pl.pallas_call(
        image_kernel,
        in_specs=[SCALAR, kept, kept, kept],
        out_specs=[kept] * (ny + 2),
        out_shape=[some, half, half] + [piece] * (ny - 1),
        scratch_shapes=[pltpu.VMEM((perts, nx * share, rows), NARROW)],
        compiler_params=ROOMY,
    )(at, other, perturbation, own_image)
    down, up = turn(first, "y", 1), turn(last, "y", -1)
    down = jnp.pad(down, [(0, block), (0, 0)])
    up = jnp.pad(up, [(block, 0), (0, 0)])
    for d in range(ny // 2 - 1, 0, -1):
        down = turn((near[d].astype(WIDE) + down).astype(NARROW), "y", 1)
        up = turn((near[-d].astype(WIDE) + up).astype(NARROW), "y", -1)

    wide_occ = up_to(own_occ, LANES)
    send, keep, far = pl.pallas_call(
        coupling_kernel,
        in_specs=[SCALAR] + [kept] * (3 + len(occ)),
        out_specs=[kept] * 3,
        out_shape=[
            shape_of(ny, block, wide_occ),
            shape_of(ny, block, wide_occ, dtype=WIDE),
            shape_of(*occ_coeffs.shape),
        ],
        scratch_shapes=[pltpu.VMEM((perts * block, rows), NARROW)],
        compiler_params=ROOMY,
    )(at, near[0], down, up, *occ)
    terms = (keep + lax.ppermute(send, "k", SWAP)).astype(NARROW)
    terms = exchanged(terms, "x")

    chunk = (y + jnp.array(ring_order(ny), jnp.int32)[x]) % ny
    levels = jnp.pad(occ_energies.reshape(ny, own_occ), [(0, 0), (0, wide_occ - own_occ)], constant_values=-1.0)
    levels = lax.dynamic_slice_in_dim(levels, chunk, 1, 0)
    virtual = lax.dynamic_slice_in_dim(vir_energies, y * block, block, 0)[:, None]
    response = pl.pallas_call(
        response_kernel, out_shape=shape_of(nx, block, wide_occ), compiler_params=ROOMY
    )(terms, levels, virtual)
    response = exchanged(response, "x")
    sibling = lax.ppermute(response, "k", SWAP)
    mixed = pl.pallas_call(
        mixed_kernel,
        in_specs=[SCALAR] + [kept] * (1 + len(occ)),
        out_specs=kept,
        out_shape=piece,
        compiler_params=ROOMY,
    )(at, response, sibling, *occ[:-2], far)

    pieces = ring_gather(mixed, "y", block)
    tile = 2 * LANES
    total = pl.pallas_call(
        density_kernel,
        grid=(pl.cdiv(rows, tile),),
        in_specs=[SCALAR] + [kept] * (2 + len(pieces)),
        out_specs=pl.BlockSpec((tile, perts, cols), lambda i: (i, 0, 0)),
        out_shape=shape_of(rows, perts, cols),
        compiler_params=ROOMY,
    )(at, turned, other_turned, *pieces)
    return jnp.transpose(total, (1, 0, 2))


def solution(mesh):
    rows, cols = mesh.shape["row"], mesh.shape["col"]
    torus = Mesh(
        mesh.devices.reshape(mesh.shape["grp"], rows // CORES, CORES, cols),
        ("grp", "x", "k", "y"),
    )
    row = ("x", "k")
    in_specs = (P("grp", row, "y"), P(row, "y"), P("y", row), P(), P())

    return jax.shard_map(per_device, mesh=torus, in_specs=in_specs, out_specs=P("grp", row, "y"), check_vma=False)
```

```python
import functools

import jax
import jax.numpy as jnp
from jax import lax
from jax.experimental import pallas as pl
from jax.experimental.pallas import tpu as pltpu
from jax.sharding import Mesh
from jax.sharding import PartitionSpec as P

CORES = 2
LANES = 128
SWAP = [(0, 1), (1, 0)]
WIDE, NARROW = jnp.float32, jnp.bfloat16
ROOMY = pltpu.CompilerParams(vmem_limit_bytes=20 * 2**20)
SCALAR = pl.BlockSpec(memory_space=pltpu.SMEM)


def up_to(size, unit):
    return -(-size // unit) * unit


def shape_of(*dims, dtype=NARROW):
    return jax.ShapeDtypeStruct(dims, dtype)


def turn(shard, axis, step):
    size = lax.axis_size(axis)
    return lax.ppermute(shard, axis, [(i, (i + step) % size) for i in range(size)])


def ring_gather(shard, axis, mid):
    half = lax.axis_size(axis) // 2
    pieces, down, up = [shard], shard, shard
    for _ in range(half - 1):
        down, up = turn(down, axis, 1), turn(up, axis, -1)
        pieces += [down, up]
    far = [turn(down[:mid], axis, 1), turn(up[mid:], axis, -1)]
    return pieces + far


def ring_order(size):
    steps = [0]
    for s in range(1, size // 2):
        steps += [size - s, s]
    return steps + [size // 2]


def exchanged(pieces, axis):
    return lax.all_to_all(pieces, axis, split_axis=0, concat_axis=0, tiled=True)


def dot(a, b, over):
    return lax.dot_general(a, b, ((over[:1], over[1:]), ((), ())), preferred_element_type=WIDE)


def turn_and_multiply(at, held, pert, turned, image):
    size, share, _ = held.shape
    for d in range(size):
        turned[d * share : (d + 1) * share, :] = held[lax.rem(at[0] + d, size)]
    for p in range(pert.shape[0]):
        image[p] = dot(turned[...], pert[p], (1, 1)).astype(NARROW)


def own_image_kernel(at, held, pert, turned, image):
    turn_and_multiply(at, held, pert, turned, image)


def image_kernel(at, held, pert, own_image, turned, first, last, *refs):
    *near, image = refs
    turn_and_multiply(at, held, pert, turned, image)
    k = at[1]
    size, share, _ = held.shape
    for p in range(pert.shape[0]):
        for d in range(size):
            for core, source in ((k, own_image), (1 - k, image)):
                part = source[p, d * share : (d + 1) * share, :]
                start = pl.multiple_of(core * share, share)
                if d == size // 2:
                    (first, last)[p][pl.ds(start, share), :] = part
                else:
                    near[d - (d > size // 2)][pl.ds(CORES * p * share + start, share), :] = part


def coupling_kernel(at, here, down, up, *refs):
    *chunks, far_low, far_high, send, keep, far, image = refs
    k = at[1]
    far[: far_low.shape[0], :] = far_low[...]
    far[far_low.shape[0] :, :] = far_high[...]
    image[...] = (here[...].astype(WIDE) + down[...].astype(WIDE) + up[...].astype(WIDE)).astype(NARROW)
    block = image.shape[0] // CORES
    held = [image[pl.ds(pl.multiple_of(c * block, block), block), :] for c in (1 - k, k)]
    left = jnp.concatenate(held, axis=0)
    chunks = [c[...] for c in (*chunks, far)]
    width = chunks[0].shape[1]
    spare = send.shape[2] - width
    for n, chunk in enumerate(chunks):
        value = dot(left, chunk, (1, 0))
        send[n, :, :width] = value[:block].astype(NARROW)
        keep[n, :, :width] = value[block:]
        send[n, :, width:] = jnp.zeros((block, spare), NARROW)
        keep[n, :, width:] = jnp.zeros((block, spare), WIDE)


def response_kernel(terms, levels, virtual, out):
    coupling = terms[0].astype(WIDE)
    for n in range(1, terms.shape[0]):
        coupling += terms[n].astype(WIDE)
    response = (coupling / (levels[...] - virtual[...])).astype(NARROW)
    for n in range(out.shape[0]):
        out[n] = response


def mixed_kernel(at, own, other, *refs):
    *chunks, out = refs
    k = at[1]
    chunks = [c[...] for c in chunks]
    width = chunks[0].shape[1]
    total = 0.0
    for n, chunk in enumerate(chunks):
        left = jnp.concatenate([own[n], other[n]], axis=0)[:, :width]
        total += dot(left, chunk, (1, 1))
    block = own.shape[1]
    total = total.astype(NARROW)
    for core, part in ((k, total[:block]), (1 - k, total[block:])):
        out[pl.ds(pl.multiple_of(core * block, block), block), :] = part


def density_kernel(at, turned, other_turned, *refs):
    *pieces, first, last, out, whole = refs
    k = at[1]
    size = len(pieces) + 1
    block = first.shape[0]
    share = block // CORES
    rows, tile = first.shape[1], out.shape[0]

    @pl.when(pl.program_id(0) == 0)
    def _():
        whole[: size * share, :] = turned[...]
        whole[size * share :, :] = other_turned[...]

    def stretch(low, high):
        for p in range(out.shape[1]):
            left = []
            for core in (k, 1 - k):
                start = pl.multiple_of(core * share, share)
                near = pl.ds(p * block + start, share)
                at_block = {d: piece[near, low:high] for d, piece in zip(ring_order(size), pieces)}
                at_block[size // 2] = (first, last)[p][pl.ds(start, share), low:high]
                left += [at_block[d] for d in range(size)]
            left = jnp.concatenate(left, axis=0)
            out[: high - low, p, :] = dot(left, whole[...], (0, 0)).astype(NARROW)

    for n, low in enumerate(range(0, rows, tile)):
        pl.when(pl.program_id(0) == n)(functools.partial(stretch, low, min(low + tile, rows)))


def per_device(perturbation, occ_coeffs, vir_coeffs, occ_energies, vir_energies):
    nx, ny = lax.axis_size("x"), lax.axis_size("y")
    x, k, y = (lax.axis_index(a) for a in ("x", "k", "y"))
    perts, rows, cols = perturbation.shape
    own_occ = occ_coeffs.shape[1]
    share = vir_coeffs.shape[1]
    block = CORES * share
    at = jnp.stack([y, k]).astype(jnp.int32)

    mid = up_to(rows // 2, LANES)
    occ = ring_gather(occ_coeffs, "y", mid)
    own = exchanged(jnp.broadcast_to(vir_coeffs.T, (nx, share, cols)), "x")
    other = lax.ppermute(own, "k", SWAP)

    piece = shape_of(perts * block, rows)
    half = shape_of(block, rows)
    kept = pl.BlockSpec(memory_space=pltpu.VMEM)
    some = shape_of(nx * share, cols)
    turned, own_image = pl.pallas_call(
        own_image_kernel,
        in_specs=[SCALAR, kept, kept],
        out_specs=[kept, kept],
        out_shape=[some, shape_of(perts, nx * share, rows)],
        compiler_params=ROOMY,
    )(at, own, perturbation)
    other_turned, first, last, *near = pl.pallas_call(
        image_kernel,
        in_specs=[SCALAR, kept, kept, kept],
        out_specs=[kept] * (ny + 2),
        out_shape=[some, half, half] + [piece] * (ny - 1),
        scratch_shapes=[pltpu.VMEM((perts, nx * share, rows), NARROW)],
        compiler_params=ROOMY,
    )(at, other, perturbation, own_image)
    down, up = turn(first, "y", 1), turn(last, "y", -1)
    down = jnp.pad(down, [(0, block), (0, 0)])
    up = jnp.pad(up, [(block, 0), (0, 0)])
    for d in range(ny // 2 - 1, 0, -1):
        down = turn((near[d].astype(WIDE) + down).astype(NARROW), "y", 1)
        up = turn((near[-d].astype(WIDE) + up).astype(NARROW), "y", -1)

    wide_occ = up_to(own_occ, LANES)
    send, keep, far = pl.pallas_call(
        coupling_kernel,
        in_specs=[SCALAR] + [kept] * (3 + len(occ)),
        out_specs=[kept] * 3,
        out_shape=[
            shape_of(ny, block, wide_occ),
            shape_of(ny, block, wide_occ, dtype=WIDE),
            shape_of(*occ_coeffs.shape),
        ],
        scratch_shapes=[pltpu.VMEM((perts * block, rows), NARROW)],
        compiler_params=ROOMY,
    )(at, near[0], down, up, *occ)
    terms = (keep + lax.ppermute(send, "k", SWAP)).astype(NARROW)
    terms = exchanged(terms, "x")

    chunk = (y + jnp.array(ring_order(ny), jnp.int32)[x]) % ny
    levels = jnp.pad(occ_energies.reshape(ny, own_occ), [(0, 0), (0, wide_occ - own_occ)], constant_values=-1.0)
    levels = lax.dynamic_slice_in_dim(levels, chunk, 1, 0)
    virtual = lax.dynamic_slice_in_dim(vir_energies, y * block, block, 0)[:, None]
    response = pl.pallas_call(
        response_kernel, out_shape=shape_of(nx, block, wide_occ), compiler_params=ROOMY
    )(terms, levels, virtual)
    response = exchanged(response, "x")
    sibling = lax.ppermute(response, "k", SWAP)
    mixed = pl.pallas_call(
        mixed_kernel,
        in_specs=[SCALAR] + [kept] * (1 + len(occ)),
        out_specs=kept,
        out_shape=piece,
        compiler_params=ROOMY,
    )(at, response, sibling, *occ[:-2], far)

    pieces = ring_gather(mixed, "y", block)
    tile = 2 * LANES
    total = pl.pallas_call(
        density_kernel,
        grid=(pl.cdiv(rows, tile),),
        in_specs=[SCALAR] + [kept] * (2 + len(pieces)),
        out_specs=pl.BlockSpec((tile, perts, cols), lambda i: (i, 0, 0)),
        out_shape=shape_of(rows, perts, cols),
        scratch_shapes=[pltpu.VMEM((nx * block, cols), NARROW)],
        compiler_params=ROOMY,
    )(at, turned, other_turned, *pieces)
    return jnp.transpose(total, (1, 0, 2))


def solution(mesh):
    rows, cols = mesh.shape["row"], mesh.shape["col"]
    torus = Mesh(
        mesh.devices.reshape(mesh.shape["grp"], rows // CORES, CORES, cols),
        ("grp", "x", "k", "y"),
    )
    row = ("x", "k")
    in_specs = (P("grp", row, "y"), P(row, "y"), P("y", row), P(), P())

    return jax.shard_map(per_device, mesh=torus, in_specs=in_specs, out_specs=P("grp", row, "y"), check_vma=False)
```

```python
import jax
import jax.numpy as jnp
from jax import lax
from jax.experimental import pallas as pl
from jax.experimental.pallas import tpu as pltpu
from jax.sharding import Mesh
from jax.sharding import PartitionSpec as P

CORES = 2
LANES = 128
SWAP = [(0, 1), (1, 0)]
WIDE, NARROW = jnp.float32, jnp.bfloat16
ROOMY = pltpu.CompilerParams(vmem_limit_bytes=20 * 2**20)
SCALAR = pl.BlockSpec(memory_space=pltpu.SMEM)


def up_to(size, unit):
    return -(-size // unit) * unit


def shape_of(*dims, dtype=NARROW):
    return jax.ShapeDtypeStruct(dims, dtype)


def turn(shard, axis, step):
    size = lax.axis_size(axis)
    return lax.ppermute(shard, axis, [(i, (i + step) % size) for i in range(size)])


def ring_gather(shard, axis, mid):
    half = lax.axis_size(axis) // 2
    pieces, down, up = [shard], shard, shard
    for _ in range(half - 1):
        down, up = turn(down, axis, 1), turn(up, axis, -1)
        pieces += [down, up]
    far = [turn(down[:mid], axis, 1), turn(up[mid:], axis, -1)]
    return pieces + far


def ring_order(size):
    steps = [0]
    for s in range(1, size // 2):
        steps += [size - s, s]
    return steps + [size // 2]


def exchanged(pieces, axis):
    return lax.all_to_all(pieces, axis, split_axis=0, concat_axis=0, tiled=True)


def dot(a, b, over):
    return lax.dot_general(a, b, ((over[:1], over[1:]), ((), ())), preferred_element_type=WIDE)


def copies_kernel(shard, out, sent):
    copies = [pltpu.make_async_copy(shard, out.at[n], sent.at[n]) for n in range(out.shape[0])]
    for copy in copies:
        copy.start()
    for copy in copies:
        copy.wait()


def turn_and_multiply(at, held, pert, turned, image):
    size, share, _ = held.shape
    for d in range(size):
        turned[d * share : (d + 1) * share, :] = held[lax.rem(at[0] + d, size)]

    @pl.loop(0, pert.shape[0])
    def _(p):
        image[p] = dot(turned[...], pert[p], (1, 1)).astype(NARROW)


def own_image_kernel(at, held, pert, turned, image):
    turn_and_multiply(at, held, pert, turned, image)


def image_kernel(at, held, pert, own_image, turned, first, last, *refs):
    *near, image = refs
    turn_and_multiply(at, held, pert, turned, image)
    k = at[1]
    size, share, _ = held.shape
    for p in range(pert.shape[0]):
        for d in range(size):
            for core, source in ((k, own_image), (1 - k, image)):
                part = source[p, d * share : (d + 1) * share, :]
                start = pl.multiple_of(core * share, share)
                if d == size // 2:
                    (first, last)[p][pl.ds(start, share), :] = part
                else:
                    near[d - (d > size // 2)][pl.ds(CORES * p * share + start, share), :] = part


def coupling_kernel(at, here, down, up, *refs):
    *chunks, far_low, far_high, send, keep, far, image = refs
    k = at[1]
    far[: far_low.shape[0], :] = far_low[...]
    far[far_low.shape[0] :, :] = far_high[...]
    image[...] = (here[...].astype(WIDE) + down[...].astype(WIDE) + up[...].astype(WIDE)).astype(NARROW)
    block = image.shape[0] // CORES
    held = [image[pl.ds(pl.multiple_of(c * block, block), block), :] for c in (1 - k, k)]
    left = jnp.concatenate(held, axis=0)
    chunks = [c[...] for c in (*chunks, far)]
    width = chunks[0].shape[1]
    spare = send.shape[2] - width
    for n, chunk in enumerate(chunks):
        value = dot(left, chunk, (1, 0))
        send[n, :, :width] = value[:block].astype(NARROW)
        keep[n, :, :width] = value[block:]
        send[n, :, width:] = jnp.zeros((block, spare), NARROW)
        keep[n, :, width:] = jnp.zeros((block, spare), WIDE)


def response_kernel(terms, levels, virtual, out):
    coupling = terms[0].astype(WIDE)
    for n in range(1, terms.shape[0]):
        coupling += terms[n].astype(WIDE)
    response = (coupling / (levels[...] - virtual[...])).astype(NARROW)
    for n in range(out.shape[0]):
        out[n] = response


def mixed_kernel(response, *refs):
    *chunks, out = refs
    width = chunks[0].shape[1]
    total = 0.0
    for n, chunk in enumerate(chunks):
        total += dot(response[n][:, :width], chunk[...], (1, 1))
    out[...] = total.astype(NARROW)


def join_kernel(low, high, out):
    out[: low.shape[0], :] = low[...]
    out[low.shape[0] :, :] = high[...]


def density_kernel(at, turned, *refs):
    *refs, out = refs
    k = at[1]
    perts = out.shape[1]
    group = len(refs) // perts
    size = group - 1
    block, rows = refs[0].shape
    share, tile = block // CORES, out.shape[0]

    def stretch(low, width):
        lanes = pl.ds(low, width)
        waves = []
        for w in range(perts):
            *pieces, first, last = refs[w * group : (w + 1) * group]
            at_block = {d: piece[:, lanes] for d, piece in zip(ring_order(size), pieces)}
            at_block[size // 2] = jnp.concatenate([first[:, lanes], last[:, lanes]], axis=0)
            waves.append(at_block)
        for p in range(perts):
            mine, yours = waves
            block_of = {d: jnp.where(k == p, mine[d], yours[d]) for d in range(size)}
            left = [block_of[d][:share] for d in range(size)], [block_of[d][share:] for d in range(size)]
            ahead = [jnp.where(k == 0, a, b) for a, b in zip(*left)]
            left = jnp.concatenate(ahead + [jnp.where(k == 0, b, a) for a, b in zip(*left)], axis=0)
            out[:width, p, :] = dot(left, turned[...], (0, 0)).astype(NARROW)

    step, whole = pl.program_id(0), rows // tile

    @pl.when(step < whole)
    def _():
        stretch(pl.multiple_of(step * tile, tile), tile)

    @pl.when(step >= whole)
    def _():
        stretch(whole * tile, rows - whole * tile)


def per_device(perturbation, occ_coeffs, vir_coeffs, occ_energies, vir_energies):
    nx, ny = lax.axis_size("x"), lax.axis_size("y")
    x, k, y = (lax.axis_index(a) for a in ("x", "k", "y"))
    perts, rows, cols = perturbation.shape
    own_occ = occ_coeffs.shape[1]
    share = vir_coeffs.shape[1]
    block = CORES * share
    at = jnp.stack([y, k]).astype(jnp.int32)

    mid = up_to(rows // 2, LANES)
    occ = ring_gather(occ_coeffs, "y", mid)
    anywhere = pl.BlockSpec(memory_space=pl.ANY)
    own = pl.pallas_call(
        copies_kernel,
        in_specs=[anywhere],
        out_specs=anywhere,
        out_shape=shape_of(nx, share, cols),
        scratch_shapes=[pltpu.SemaphoreType.DMA((nx,))],
    )(vir_coeffs.T)
    own = exchanged(own, "x")
    other = lax.ppermute(own, "k", SWAP)

    piece = shape_of(perts * block, rows)
    half = shape_of(block, rows)
    kept = pl.BlockSpec(memory_space=pltpu.VMEM)
    some = shape_of(nx * share, cols)
    turned, own_image = pl.pallas_call(
        own_image_kernel,
        in_specs=[SCALAR, kept, kept],
        out_specs=[kept, kept],
        out_shape=[some, shape_of(perts, nx * share, rows)],
        compiler_params=ROOMY,
    )(at, own, perturbation)
    other_turned, first, last, *near = pl.pallas_call(
        image_kernel,
        in_specs=[SCALAR, kept, kept, kept],
        out_specs=[kept] * (ny + 2),
        out_shape=[some, half, half] + [piece] * (ny - 1),
        scratch_shapes=[pltpu.VMEM((perts, nx * share, rows), NARROW)],
        compiler_params=ROOMY,
    )(at, other, perturbation, own_image)
    down, up = turn(first, "y", 1), turn(last, "y", -1)
    down = jnp.pad(down, [(0, block), (0, 0)])
    up = jnp.pad(up, [(block, 0), (0, 0)])
    for d in range(ny // 2 - 1, 0, -1):
        down = turn((near[d].astype(WIDE) + down).astype(NARROW), "y", 1)
        up = turn((near[-d].astype(WIDE) + up).astype(NARROW), "y", -1)

    wide_occ = up_to(own_occ, LANES)
    send, keep, far = pl.pallas_call(
        coupling_kernel,
        in_specs=[SCALAR] + [kept] * (3 + len(occ)),
        out_specs=[kept] * 3,
        out_shape=[
            shape_of(ny, block, wide_occ),
            shape_of(ny, block, wide_occ, dtype=WIDE),
            shape_of(*occ_coeffs.shape),
        ],
        scratch_shapes=[pltpu.VMEM((perts * block, rows), NARROW)],
        compiler_params=ROOMY,
    )(at, near[0], down, up, *occ)
    terms = (keep + lax.ppermute(send, "k", SWAP)).astype(NARROW)
    terms = exchanged(terms, "x")

    chunk = (y + jnp.array(ring_order(ny), jnp.int32)[x]) % ny
    levels = jnp.pad(occ_energies.reshape(ny, own_occ), [(0, 0), (0, wide_occ - own_occ)], constant_values=-1.0)
    levels = lax.dynamic_slice_in_dim(levels, chunk, 1, 0)
    virtual = lax.dynamic_slice_in_dim(vir_energies, y * block, block, 0)[:, None]
    response = pl.pallas_call(
        response_kernel, out_shape=shape_of(nx, block, wide_occ), compiler_params=ROOMY
    )(terms, levels, virtual)
    response = exchanged(response, "x")
    sibling = lax.ppermute(response, "k", SWAP)
    pieces = []
    for part in (response, sibling):
        mixed = pl.pallas_call(
            mixed_kernel,
            in_specs=[kept] * (1 + ny),
            out_specs=kept,
            out_shape=half,
            compiler_params=ROOMY,
        )(part, *occ[:-2], far)
        pieces += ring_gather(mixed, "y", share)
    turned = pl.pallas_call(
        join_kernel,
        in_specs=[kept] * 2,
        out_specs=kept,
        out_shape=shape_of(nx * block, cols),
        compiler_params=ROOMY,
    )(turned, other_turned)
    tile = 2 * LANES
    total = pl.pallas_call(
        density_kernel,
        grid=(pl.cdiv(rows, tile),),
        in_specs=[SCALAR] + [kept] * (1 + len(pieces)),
        out_specs=pl.BlockSpec((tile, perts, cols), lambda i: (i, 0, 0)),
        out_shape=shape_of(rows, perts, cols),
        compiler_params=ROOMY,
    )(at, turned, *pieces)
    return jnp.transpose(total, (1, 0, 2))


def solution(mesh):
    rows, cols = mesh.shape["row"], mesh.shape["col"]
    torus = Mesh(
        mesh.devices.reshape(mesh.shape["grp"], rows // CORES, CORES, cols),
        ("grp", "x", "k", "y"),
    )
    row = ("x", "k")
    in_specs = (P("grp", row, "y"), P(row, "y"), P("y", row), P(), P())

    return jax.shard_map(per_device, mesh=torus, in_specs=in_specs, out_specs=P("grp", row, "y"), check_vma=False)
```

```python
import jax
import jax.numpy as jnp
from jax import lax
from jax.experimental import pallas as pl
from jax.experimental.pallas import tpu as pltpu
from jax.sharding import Mesh
from jax.sharding import PartitionSpec as P

CORES = 2
LANES = 128
SWAP = [(0, 1), (1, 0)]
WIDE, NARROW = jnp.float32, jnp.bfloat16
ROOMY = pltpu.CompilerParams(vmem_limit_bytes=20 * 2**20)
SCALAR = pl.BlockSpec(memory_space=pltpu.SMEM)


def up_to(size, unit):
    return -(-size // unit) * unit


def shape_of(*dims, dtype=NARROW):
    return jax.ShapeDtypeStruct(dims, dtype)


def turn(shard, axis, step):
    size = lax.axis_size(axis)
    return lax.ppermute(shard, axis, [(i, (i + step) % size) for i in range(size)])


def ring_gather(shard, axis, mid):
    half = lax.axis_size(axis) // 2
    pieces, down, up = [shard], shard, shard
    for _ in range(half - 1):
        down, up = turn(down, axis, 1), turn(up, axis, -1)
        pieces += [down, up]
    far = [turn(down[:mid], axis, 1), turn(up[mid:], axis, -1)]
    return pieces + far


def ring_order(size):
    steps = [0]
    for s in range(1, size // 2):
        steps += [size - s, s]
    return steps + [size // 2]


def exchanged(pieces, axis):
    return lax.all_to_all(pieces, axis, split_axis=0, concat_axis=0, tiled=True)


def dot(a, b, over):
    return lax.dot_general(a, b, ((over[:1], over[1:]), ((), ())), preferred_element_type=WIDE)


def turn_and_multiply(at, held, pert, turned, image):
    size, share, _ = held.shape
    for d in range(size):
        turned[d * share : (d + 1) * share, :] = held[lax.rem(at[0] + d, size)]
    for p in range(pert.shape[0]):
        image[p] = dot(turned[...], pert[p], (1, 1)).astype(NARROW)


def own_image_kernel(at, held, pert, turned, image):
    turn_and_multiply(at, held, pert, turned, image)


def image_kernel(at, held, pert, own_image, turned, first, last, *refs):
    *near, image = refs
    turn_and_multiply(at, held, pert, turned, image)
    k = at[1]
    size, share, _ = held.shape
    for p in range(pert.shape[0]):
        for d in range(size):
            for core, source in ((k, own_image), (1 - k, image)):
                part = source[p, d * share : (d + 1) * share, :]
                start = pl.multiple_of(core * share, share)
                if d == size // 2:
                    (first, last)[p][pl.ds(start, share), :] = part
                else:
                    near[d - (d > size // 2)][pl.ds(CORES * p * share + start, share), :] = part


def coupling_kernel(at, here, down, up, *refs):
    *chunks, far_low, far_high, send, keep, far, image = refs
    k = at[1]
    far[: far_low.shape[0], :] = far_low[...]
    far[far_low.shape[0] :, :] = far_high[...]
    image[...] = (here[...].astype(WIDE) + down[...].astype(WIDE) + up[...].astype(WIDE)).astype(NARROW)
    block = image.shape[0] // CORES
    held = [image[pl.ds(pl.multiple_of(c * block, block), block), :] for c in (1 - k, k)]
    left = jnp.concatenate(held, axis=0)
    chunks = [c[...] for c in (*chunks, far)]
    width = chunks[0].shape[1]
    spare = send.shape[2] - width
    for n, chunk in enumerate(chunks):
        value = dot(left, chunk, (1, 0))
        send[n, :, :width] = value[:block].astype(NARROW)
        keep[n, :, :width] = value[block:]
        send[n, :, width:] = jnp.zeros((block, spare), NARROW)
        keep[n, :, width:] = jnp.zeros((block, spare), WIDE)


def response_kernel(terms, levels, virtual, out):
    coupling = terms[0].astype(WIDE)
    for n in range(1, terms.shape[0]):
        coupling += terms[n].astype(WIDE)
    response = (coupling / (levels[...] - virtual[...])).astype(NARROW)
    for n in range(out.shape[0]):
        out[n] = response


def mixed_kernel(response, *refs):
    *chunks, out = refs
    width = chunks[0].shape[1]
    total = 0.0
    for n, chunk in enumerate(chunks):
        total += dot(response[n][:, :width], chunk[...], (1, 1))
    rows = total.shape[1]
    out[:, :rows] = total.astype(NARROW)
    out[:, rows:] = jnp.zeros((out.shape[0], out.shape[1] - rows), NARROW)


def join_kernel(at, mine, yours, out):
    k = at[1]
    size, _, share, _ = out.shape
    for core, held in ((k, mine), (1 - k, yours)):
        for d in range(size):
            out[d, core] = held[d * share : (d + 1) * share, :]


def density_kernel(at, turned, *refs):
    *refs, out = refs
    k = at[1]
    perts = out.shape[1]
    group = len(refs) // perts
    size = group - 1
    tile = out.shape[0]
    lanes = pl.ds(pl.multiple_of(pl.program_id(0) * tile, tile), tile)
    waves = []
    for w in range(perts):
        *pieces, first, last = refs[w * group : (w + 1) * group]
        at_block = {d: piece[:, lanes] for d, piece in zip(ring_order(size), pieces)}
        at_block[size // 2] = jnp.concatenate([first[:, lanes], last[:, lanes]], axis=0)
        waves.append(at_block)
    mine, yours = waves
    for p in range(perts):
        left = [jnp.where(k == p, mine[d], yours[d]) for d in range(size)]
        total = dot(jnp.concatenate(left, axis=0), turned[...], (0, 0))
        out[:, p, :] = total.astype(NARROW)


def per_device(perturbation, occ_coeffs, vir_coeffs, occ_energies, vir_energies):
    nx, ny = lax.axis_size("x"), lax.axis_size("y")
    x, k, y = (lax.axis_index(a) for a in ("x", "k", "y"))
    perts, rows, cols = perturbation.shape
    own_occ = occ_coeffs.shape[1]
    share = vir_coeffs.shape[1]
    block = CORES * share
    at = jnp.stack([y, k]).astype(jnp.int32)

    mid = up_to(rows // 2, LANES)
    occ = ring_gather(occ_coeffs, "y", mid)
    own = exchanged(jnp.broadcast_to(vir_coeffs.T, (nx, share, cols)), "x")
    other = lax.ppermute(own, "k", SWAP)

    piece = shape_of(perts * block, rows)
    half = shape_of(block, rows)
    kept = pl.BlockSpec(memory_space=pltpu.VMEM)
    some = shape_of(nx * share, cols)
    turned, own_image = pl.pallas_call(
        own_image_kernel,
        in_specs=[SCALAR, kept, kept],
        out_specs=[kept, kept],
        out_shape=[some, shape_of(perts, nx * share, rows)],
        compiler_params=ROOMY,
    )(at, own, perturbation)
    other_turned, first, last, *near = pl.pallas_call(
        image_kernel,
        in_specs=[SCALAR, kept, kept, kept],
        out_specs=[kept] * (ny + 2),
        out_shape=[some, half, half] + [piece] * (ny - 1),
        scratch_shapes=[pltpu.VMEM((perts, nx * share, rows), NARROW)],
        compiler_params=ROOMY,
    )(at, other, perturbation, own_image)
    down, up = turn(first, "y", 1), turn(last, "y", -1)
    down = jnp.pad(down, [(0, block), (0, 0)])
    up = jnp.pad(up, [(block, 0), (0, 0)])
    for d in range(ny // 2 - 1, 0, -1):
        down = turn((near[d].astype(WIDE) + down).astype(NARROW), "y", 1)
        up = turn((near[-d].astype(WIDE) + up).astype(NARROW), "y", -1)

    wide_occ = up_to(own_occ, LANES)
    send, keep, far = pl.pallas_call(
        coupling_kernel,
        in_specs=[SCALAR] + [kept] * (3 + len(occ)),
        out_specs=[kept] * 3,
        out_shape=[
            shape_of(ny, block, wide_occ),
            shape_of(ny, block, wide_occ, dtype=WIDE),
            shape_of(*occ_coeffs.shape),
        ],
        scratch_shapes=[pltpu.VMEM((perts * block, rows), NARROW)],
        compiler_params=ROOMY,
    )(at, near[0], down, up, *occ)
    terms = (keep + lax.ppermute(send, "k", SWAP)).astype(NARROW)
    terms = exchanged(terms, "x")

    chunk = (y + jnp.array(ring_order(ny), jnp.int32)[x]) % ny
    levels = jnp.pad(occ_energies.reshape(ny, own_occ), [(0, 0), (0, wide_occ - own_occ)], constant_values=-1.0)
    levels = lax.dynamic_slice_in_dim(levels, chunk, 1, 0)
    virtual = lax.dynamic_slice_in_dim(vir_energies, y * block, block, 0)[:, None]
    response = pl.pallas_call(
        response_kernel, out_shape=shape_of(nx, block, wide_occ), compiler_params=ROOMY
    )(terms, levels, virtual)
    response = exchanged(response, "x")
    sibling = lax.ppermute(response, "k", SWAP)
    tile = 2 * LANES
    pieces = []
    for part in (response, sibling):
        mixed = pl.pallas_call(
            mixed_kernel,
            in_specs=[kept] * (1 + ny),
            out_specs=kept,
            out_shape=shape_of(block, up_to(rows, tile)),
            compiler_params=ROOMY,
        )(part, *occ[:-2], far)
        pieces += ring_gather(mixed, "y", share)
    turned = pl.pallas_call(
        join_kernel,
        in_specs=[SCALAR, kept, kept],
        out_specs=kept,
        out_shape=shape_of(nx, CORES, share, cols),
        compiler_params=ROOMY,
    )(at, turned, other_turned).reshape(nx * block, cols)
    total = pl.pallas_call(
        density_kernel,
        grid=(pl.cdiv(rows, tile),),
        in_specs=[SCALAR] + [kept] * (1 + len(pieces)),
        out_specs=pl.BlockSpec((tile, perts, cols), lambda i: (i, 0, 0)),
        out_shape=shape_of(rows, perts, cols),
        compiler_params=ROOMY,
    )(at, turned, *pieces)
    return jnp.transpose(total, (1, 0, 2))


def solution(mesh):
    rows, cols = mesh.shape["row"], mesh.shape["col"]
    torus = Mesh(
        mesh.devices.reshape(mesh.shape["grp"], rows // CORES, CORES, cols),
        ("grp", "x", "k", "y"),
    )
    row = ("x", "k")
    in_specs = (P("grp", row, "y"), P(row, "y"), P("y", row), P(), P())

    return jax.shard_map(per_device, mesh=torus, in_specs=in_specs, out_specs=P("grp", row, "y"), check_vma=False)
```

```python
import functools

import jax
import jax.numpy as jnp
from jax import lax
from jax.experimental import pallas as pl
from jax.experimental.pallas import tpu as pltpu
from jax.sharding import Mesh
from jax.sharding import PartitionSpec as P

CORES = 2
LANES = 128
SWAP = [(0, 1), (1, 0)]
WIDE, NARROW = jnp.float32, jnp.bfloat16
ROOMY = pltpu.CompilerParams(vmem_limit_bytes=20 * 2**20)
SCALAR = pl.BlockSpec(memory_space=pltpu.SMEM)


def up_to(size, unit):
    return -(-size // unit) * unit


def shape_of(*dims, dtype=NARROW):
    return jax.ShapeDtypeStruct(dims, dtype)


def turn(shard, axis, step):
    size = lax.axis_size(axis)
    return lax.ppermute(shard, axis, [(i, (i + step) % size) for i in range(size)])


def ring_gather(shard, axis, mid, straight=False):
    half = lax.axis_size(axis) // 2
    pieces, down, up = [shard], shard, shard
    if straight:
        far = [turn(shard[:mid], axis, half), turn(shard[mid:], axis, -half)]
    for _ in range(half - 1):
        down, up = turn(down, axis, 1), turn(up, axis, -1)
        pieces += [down, up]
    if straight:
        return pieces + far
    far = [turn(down[:mid], axis, 1), turn(up[mid:], axis, -1)]
    return pieces + far


def ring_order(size):
    steps = [0]
    for s in range(1, size // 2):
        steps += [size - s, s]
    return steps + [size // 2]


def exchanged(pieces, axis):
    return lax.all_to_all(pieces, axis, split_axis=0, concat_axis=0, tiled=True)


def dot(a, b, over):
    return lax.dot_general(a, b, ((over[:1], over[1:]), ((), ())), preferred_element_type=WIDE)


def turn_and_multiply(at, held, pert, turned, image):
    size, share, _ = held.shape
    for d in range(size):
        turned[d * share : (d + 1) * share, :] = held[lax.rem(at[0] + d, size)]
    for p in range(pert.shape[0]):
        image[p] = dot(turned[...], pert[p], (1, 1)).astype(NARROW)


def own_image_kernel(at, held, pert, turned, image):
    turn_and_multiply(at, held, pert, turned, image)


def image_kernel(at, held, pert, own_image, turned, first, last, *refs):
    *near, image = refs
    turn_and_multiply(at, held, pert, turned, image)
    k = at[1]
    size, share, _ = held.shape
    for p in range(pert.shape[0]):
        for d in range(size):
            for core, source in ((k, own_image), (1 - k, image)):
                part = source[p, d * share : (d + 1) * share, :]
                start = pl.multiple_of(core * share, share)
                if d == size // 2:
                    (first, last)[p][pl.ds(start, share), :] = part
                else:
                    near[d - (d > size // 2)][pl.ds(CORES * p * share + start, share), :] = part


def coupling_kernel(at, here, down, up, *refs):
    *chunks, far_low, far_high, send, keep, far, image = refs
    k = at[1]
    far[: far_low.shape[0], :] = far_low[...]
    far[far_low.shape[0] :, :] = far_high[...]
    image[...] = (here[...].astype(WIDE) + down[...].astype(WIDE) + up[...].astype(WIDE)).astype(NARROW)
    block = image.shape[0] // CORES
    held = [image[pl.ds(pl.multiple_of(c * block, block), block), :] for c in (1 - k, k)]
    left = jnp.concatenate(held, axis=0)
    chunks = [c[...] for c in (*chunks, far)]
    width = chunks[0].shape[1]
    spare = send.shape[2] - width
    for n, chunk in enumerate(chunks):
        value = dot(left, chunk, (1, 0))
        send[n, :, :width] = value[:block].astype(NARROW)
        keep[n, :, :width] = value[block:]
        send[n, :, width:] = jnp.zeros((block, spare), NARROW)
        keep[n, :, width:] = jnp.zeros((block, spare), WIDE)


def response_kernel(terms, levels, virtual, out):
    coupling = terms[0].astype(WIDE)
    for n in range(1, terms.shape[0]):
        coupling += terms[n].astype(WIDE)
    response = (coupling / (levels[...] - virtual[...])).astype(NARROW)
    for n in range(out.shape[0]):
        out[n] = response


def mixed_kernel(at, own, other, *refs):
    *chunks, out = refs
    k = at[1]
    chunks = [c[...] for c in chunks]
    width = chunks[0].shape[1]
    total = 0.0
    for n, chunk in enumerate(chunks):
        left = jnp.concatenate([own[n], other[n]], axis=0)[:, :width]
        total += dot(left, chunk, (1, 1))
    block = own.shape[1]
    total = total.astype(NARROW)
    for core, part in ((k, total[:block]), (1 - k, total[block:])):
        out[pl.ds(pl.multiple_of(core * block, block), block), :] = part


def density_kernel(at, turned, other_turned, *refs):
    *pieces, first, last, out, whole = refs
    k = at[1]
    size = len(pieces) + 1
    block = first.shape[0]
    share = block // CORES
    rows, tile = first.shape[1], out.shape[0]

    @pl.when(pl.program_id(0) == 0)
    def _():
        whole[: size * share, :] = turned[...]
        whole[size * share :, :] = other_turned[...]

    def stretch(low, high):
        for p in range(out.shape[1]):
            left = []
            for core in (k, 1 - k):
                start = pl.multiple_of(core * share, share)
                near = pl.ds(p * block + start, share)
                at_block = {d: piece[near, low:high] for d, piece in zip(ring_order(size), pieces)}
                at_block[size // 2] = (first, last)[p][pl.ds(start, share), low:high]
                left += [at_block[d] for d in range(size)]
            left = jnp.concatenate(left, axis=0)
            out[: high - low, p, :] = dot(left, whole[...], (0, 0)).astype(NARROW)

    for n, low in enumerate(range(0, rows, tile)):
        pl.when(pl.program_id(0) == n)(functools.partial(stretch, low, min(low + tile, rows)))


def per_device(perturbation, occ_coeffs, vir_coeffs, occ_energies, vir_energies):
    nx, ny = lax.axis_size("x"), lax.axis_size("y")
    x, k, y = (lax.axis_index(a) for a in ("x", "k", "y"))
    perts, rows, cols = perturbation.shape
    own_occ = occ_coeffs.shape[1]
    share = vir_coeffs.shape[1]
    block = CORES * share
    at = jnp.stack([y, k]).astype(jnp.int32)

    mid = up_to(rows // 2, LANES)
    occ = ring_gather(occ_coeffs, "y", mid)
    own = exchanged(jnp.broadcast_to(vir_coeffs.T, (nx, share, cols)), "x")
    other = lax.ppermute(own, "k", SWAP)

    piece = shape_of(perts * block, rows)
    half = shape_of(block, rows)
    kept = pl.BlockSpec(memory_space=pltpu.VMEM)
    some = shape_of(nx * share, cols)
    turned, own_image = pl.pallas_call(
        own_image_kernel,
        in_specs=[SCALAR, kept, kept],
        out_specs=[kept, kept],
        out_shape=[some, shape_of(perts, nx * share, rows)],
        compiler_params=ROOMY,
    )(at, own, perturbation)
    other_turned, first, last, *near = pl.pallas_call(
        image_kernel,
        in_specs=[SCALAR, kept, kept, kept],
        out_specs=[kept] * (ny + 2),
        out_shape=[some, half, half] + [piece] * (ny - 1),
        scratch_shapes=[pltpu.VMEM((perts, nx * share, rows), NARROW)],
        compiler_params=ROOMY,
    )(at, other, perturbation, own_image)
    down, up = turn(first, "y", 1), turn(last, "y", -1)
    down = jnp.pad(down, [(0, block), (0, 0)])
    up = jnp.pad(up, [(block, 0), (0, 0)])
    for d in range(ny // 2 - 1, 0, -1):
        down = turn((near[d].astype(WIDE) + down).astype(NARROW), "y", 1)
        up = turn((near[-d].astype(WIDE) + up).astype(NARROW), "y", -1)

    wide_occ = up_to(own_occ, LANES)
    send, keep, far = pl.pallas_call(
        coupling_kernel,
        in_specs=[SCALAR] + [kept] * (3 + len(occ)),
        out_specs=[kept] * 3,
        out_shape=[
            shape_of(ny, block, wide_occ),
            shape_of(ny, block, wide_occ, dtype=WIDE),
            shape_of(*occ_coeffs.shape),
        ],
        scratch_shapes=[pltpu.VMEM((perts * block, rows), NARROW)],
        compiler_params=ROOMY,
    )(at, near[0], down, up, *occ)
    terms = (keep + lax.ppermute(send, "k", SWAP)).astype(NARROW)
    terms = exchanged(terms, "x")

    chunk = (y + jnp.array(ring_order(ny), jnp.int32)[x]) % ny
    levels = jnp.pad(occ_energies.reshape(ny, own_occ), [(0, 0), (0, wide_occ - own_occ)], constant_values=-1.0)
    levels = lax.dynamic_slice_in_dim(levels, chunk, 1, 0)
    virtual = lax.dynamic_slice_in_dim(vir_energies, y * block, block, 0)[:, None]
    response = pl.pallas_call(
        response_kernel, out_shape=shape_of(nx, block, wide_occ), compiler_params=ROOMY
    )(terms, levels, virtual)
    response = exchanged(response, "x")
    sibling = lax.ppermute(response, "k", SWAP)
    mixed = pl.pallas_call(
        mixed_kernel,
        in_specs=[SCALAR] + [kept] * (1 + len(occ)),
        out_specs=kept,
        out_shape=piece,
        compiler_params=ROOMY,
    )(at, response, sibling, *occ[:-2], far)

    pieces = ring_gather(mixed, "y", block, straight=True)
    tile = 2 * LANES
    total = pl.pallas_call(
        density_kernel,
        grid=(pl.cdiv(rows, tile),),
        in_specs=[SCALAR] + [kept] * (2 + len(pieces)),
        out_specs=pl.BlockSpec((tile, perts, cols), lambda i: (i, 0, 0)),
        out_shape=shape_of(rows, perts, cols),
        scratch_shapes=[pltpu.VMEM((nx * block, cols), NARROW)],
        compiler_params=ROOMY,
    )(at, turned, other_turned, *pieces)
    return jnp.transpose(total, (1, 0, 2))


def solution(mesh):
    rows, cols = mesh.shape["row"], mesh.shape["col"]
    torus = Mesh(
        mesh.devices.reshape(mesh.shape["grp"], rows // CORES, CORES, cols),
        ("grp", "x", "k", "y"),
    )
    row = ("x", "k")
    in_specs = (P("grp", row, "y"), P(row, "y"), P("y", row), P(), P())

    return jax.shard_map(per_device, mesh=torus, in_specs=in_specs, out_specs=P("grp", row, "y"), check_vma=False)
```
